32 devices in a mesh: ea: 4 (over y, x), row: 4 (over z), col: 2 (over core).
Axes of the slice: x: 2, y: 2, z: 4, core: 2. Of those that a mesh axis runs over, the one named last changes fastest.
Arguments:
- weights: float32 [4, 256, 2048], P('ea', 'row', 'col'), parts along dimension 0, may hold values from -6 to 6
- codebook: float32 [4, 16, 2, 256], P('ea', 'col'), parts along dimension 0, may hold values from -4 to 4
- assign: int32 [4, 256, 1024], P('ea', 'row', 'col'), parts along dimension 0, may hold values from 0 to 255
- chol_upper: float32 [4, 2048, 2048], P('ea', 'row', 'col'), parts along dimension 0, may hold values from 0 to 1.4, as said below
- inv_blocks: float32 [4, 16, 128, 128], P('ea', 'col'), parts along dimension 0, may hold values from -1 to 1.5, as said below
Outputs:
- errors: float32 [4, 256, 2048], P('ea', 'row', 'col'), parts along dimension 0
- row_loss: float32 [4, 256], P('ea', 'row'), parts along dimension 0
- codeword_mass: float32 [4, 16, 256], P('ea', 'col'), parts along dimension 0
The draws below stay inside these ranges and needn't reach their ends.
There are 4 independent parts, one for each index of `ea`. The reference program is written for one: setup_inputs(seed, part) draws one part's arguments, and reference() takes and returns one part's arrays. A program takes and returns all parts, laid end to end along the dimension named above; each array names one. Nothing has to cross between parts.
Inputs may be any that keep to these rules, and one draw needn't show every extreme that they name: `chol_upper`: upper triangular with a positive diagonal. inv_blocks[x, b] is the inverse of the diagonal block of chol_upper[x] on rows and columns [b * 128, (b + 1) * 128).
All inputs are finite; a program needn't handle non-finite values.
Results may differ from the reference program's by a relative error of at most 0.0001.
Values sent between devices are 32-bit elements; how exact they have to be, the bound alone decides.
No kernel may reach another device: no remote copies, remote signals or barrier semaphores. Data moves between devices by JAX's collectives and lax.ppermute only.
A program may use at most 64 MiB of HBM per device.

```python
import jax
import jax.numpy as jnp
from jax import lax

EXP_PART = 1
COLS = 2048
BLOCK = 128
CODES = 256
ROWS = 256
NBLK = 16


def upper_factor(key):
    folded = jax.random.fold_in(key, 7)
    key_diag, key_near, key_far = jax.random.split(folded, 3)
    diagonal = jax.random.uniform(key_diag, (EXP_PART, COLS), jnp.float32, 0.7, 1.4)
    near_part = jax.random.uniform(key_near, (EXP_PART, COLS, COLS), jnp.float32, 0.0, 0.03)
    far_part = jax.random.uniform(key_far, (EXP_PART, COLS, COLS), jnp.float32, 0.0, 0.03)
    positions = jnp.arange(COLS, dtype=jnp.int32)
    same_block = positions[:, None] // BLOCK == positions[None, :] // BLOCK
    strictly_upper = positions[:, None] < positions[None, :]
    offdiag = jnp.where(same_block[None], near_part, far_part) * strictly_upper[None].astype(jnp.float32)
    return offdiag + diagonal[:, :, None] * jnp.eye(COLS, dtype=jnp.float32)[None]


def draw_chol_upper(key, part):
    return upper_factor(key)


def draw_inv_blocks(key, part):
    factor = upper_factor(key)
    blocked = factor.reshape(EXP_PART, NBLK, BLOCK, NBLK, BLOCK)
    which = jnp.arange(NBLK, dtype=jnp.int32)
    diagonal_blocks = jnp.transpose(blocked[:, which, :, which, :], (1, 0, 2, 3))
    return jnp.linalg.inv(diagonal_blocks)


def place_ends(array, key, smallest, high):
    shape = array.shape
    place = [jax.random.randint(jax.random.fold_in(key, axis), (), 0, shape[axis]) for axis in range(len(shape))]
    array = array.at[tuple(place)].set(smallest)
    longest = shape.index(max(shape))
    place[longest] = (place[longest] + 1) % shape[longest]
    return array.at[tuple(place)].set(high)


def levels(stream_key, shape, cuts, least, top_value):
    gain, own = 1.0, jax.random.fold_in(stream_key, 6)
    for axis_at, blocks in cuts:
        draws = jnp.exp(jax.random.uniform(jax.random.fold_in(own, axis_at), (blocks,), jnp.float32, least / len(cuts), top_value / len(cuts)))
        gain = gain * jnp.repeat(draws, shape[axis_at] // blocks).reshape([-1 if axis == axis_at else 1 for axis in range(len(shape))])
    return gain


def gaussian(key, dims, width, bound, shards=(), kind=jnp.bfloat16):
    drawn = width * jax.random.normal(key, dims, jnp.float32)
    if shards:
        drawn = drawn * levels(key, dims, shards, -0.22, 0.18)
    return jnp.clip(drawn, -bound, bound).astype(kind)


def setup_inputs(seed: int = 0, part: int = 0) -> dict:
    key_of = jax.random.split(jax.random.key(seed), 6)
    own_keys = jax.random.split(jax.random.fold_in(key_of[5], part), 6)
    weights = gaussian(own_keys[0], (EXP_PART, ROWS, COLS), 1.0, 6.0, ((1, 4), (2, 2)), jnp.float32)
    codebook = gaussian(own_keys[1], (EXP_PART, NBLK, 2, CODES), 1.0, 4.0, ((1, 2),), jnp.float32)
    assign = place_ends(jax.random.randint(own_keys[2], (EXP_PART, ROWS, COLS // 2), 0, CODES), jax.random.fold_in(own_keys[2], 1), 0, CODES - 1).astype(jnp.int32)
    chol_upper = draw_chol_upper(jax.random.fold_in(jax.random.fold_in(key_of[5], part), 71), part)
    inv_blocks = draw_inv_blocks(jax.random.fold_in(jax.random.fold_in(key_of[5], part), 71), part)
    return {"weights": weights, "codebook": codebook, "assign": assign, "chol_upper": chol_upper, "inv_blocks": inv_blocks}


def lookup(codebook, assign, half_block, code_count):
    pair_count = assign.shape[2]
    offsets = jnp.arange(pair_count, dtype=jnp.int32) // half_block * code_count
    flat_index = (assign + offsets[None, None, :]).astype(jnp.int32)
    experts = codebook.shape[0]
    code_table = jnp.transpose(codebook, (0, 2, 1, 3)).reshape(experts, 2, -1)

    def select(rows_table, indices):
        return jnp.stack([jnp.take(rows_table[0], indices), jnp.take(rows_table[1], indices)], axis=-1)
    picked = jax.vmap(select)(code_table, flat_index)
    return (picked.reshape(assign.shape[0], assign.shape[1], 2 * pair_count), flat_index)

def mass_by_code(errors, flat_index, segments):
    squared = errors * errors
    extent = errors.shape
    paired = squared.reshape(extent[0], extent[1], extent[2] // 2, 2).sum(axis=3)

    def summed(values, labels):
        return jax.ops.segment_sum(values.reshape(-1), labels.reshape(-1), num_segments=segments)
    return jax.vmap(summed)(paired, flat_index)

def reference(weights, codebook, assign, chol_upper, inv_blocks):
    quantized, flat_index = lookup(codebook, assign, BLOCK // 2, CODES)
    current = weights
    pieces = []
    for number in range(NBLK):
        first_col = number * BLOCK
        finish = first_col + BLOCK
        error_block = jnp.einsum('xrc,xcd->xrd', current[:, :, first_col:finish] - quantized[:, :, first_col:finish], inv_blocks[:, number], precision=lax.Precision.HIGHEST)
        pieces.append(error_block)
        if finish < COLS:
            change = jnp.einsum('xrc,xcd->xrd', error_block, chol_upper[:, first_col:finish, finish:], precision=lax.Precision.HIGHEST)
            current = jnp.concatenate([current[:, :, :finish], current[:, :, finish:] - change], axis=2)
    errors = jnp.concatenate(pieces, axis=2)
    row_loss = jnp.sum(errors * errors, axis=2)
    codeword_mass = mass_by_code(errors, flat_index, NBLK * CODES).reshape(EXP_PART, NBLK, CODES)
    return (errors, row_loss, codeword_mass)
```

```python
import jax
import jax.numpy as jnp
from jax import lax
from jax.experimental import pallas as pl
from jax.experimental.pallas import tpu as pltpu
from jax.sharding import PartitionSpec as P

LANES = 128
RADIX = 16
VMEM = pl.BlockSpec(memory_space=pltpu.VMEM)


def lane_take(values, index):
    return jnp.take_along_axis(values, index, axis=1, mode="promise_in_bounds")


def expanded_codes(codes, half, rows):
    lane = lax.broadcasted_iota(jnp.int32, (rows, LANES), 1)
    return lane_take(codes, half * (LANES // 2) + lane // 2)


def difference_kernel(weights_ref, codebook_ref, assign_ref, out_ref):
    rows = weights_ref.shape[0]
    blocks, _, code_count = codebook_ref.shape
    odd = lax.broadcasted_iota(jnp.int32, (rows, LANES), 1) % 2 == 1
    for block in range(blocks):
        lanes = pl.ds(block * LANES, LANES)
        pairs = assign_ref[:, pl.ds(block // 2 * LANES, LANES)]
        code = expanded_codes(pairs, block % 2, rows)
        low = code % LANES
        page = code // LANES
        found = jnp.zeros((rows, LANES), jnp.float32)
        for part in range(code_count // LANES):
            span = pl.ds(part * LANES, LANES)
            picked = [
                lane_take(jnp.broadcast_to(codebook_ref[block, k : k + 1, span], (rows, LANES)), low)
                for k in range(2)
            ]
            found = jnp.where(page == part, jnp.where(odd, picked[1], picked[0]), found)
        out_ref[:, lanes] = weights_ref[:, lanes] - found


def mass_kernel(errors_ref, assign_ref, out_ref, left, right):
    rows = errors_ref.shape[0]
    blocks = out_ref.shape[0]
    digits = out_ref.shape[1]
    for block in range(blocks):
        err = errors_ref[:, pl.ds(block * LANES, LANES)]
        value = err * err
        upper = value.astype(jnp.bfloat16).astype(jnp.float32)
        lower = value - upper
        code = expanded_codes(assign_ref[:, pl.ds(block // 2 * LANES, LANES)], block % 2, rows)
        high = code // RADIX
        low = code % RADIX
        digit = lax.broadcasted_iota(jnp.int32, (digits, LANES), 0)
        digit_low = lax.broadcasted_iota(jnp.int32, (RADIX, LANES), 0)
        for row in range(rows):
            one = slice(row, row + 1)
            lanes = pl.ds(row * LANES, LANES)
            hit = jnp.broadcast_to(high[one], (digits, LANES)) == digit
            left[0:digits, lanes] = jnp.where(hit, jnp.broadcast_to(upper[one], hit.shape), 0.0).astype(jnp.bfloat16)
            left[digits:, lanes] = jnp.where(hit, jnp.broadcast_to(lower[one], hit.shape), 0.0).astype(jnp.bfloat16)
            match = jnp.broadcast_to(low[one], (RADIX, LANES)) == digit_low
            right[:, lanes] = jnp.where(match, 1.0, 0.0).astype(jnp.bfloat16)
        both = lax.dot_general(
            left[...], right[...], (((1,), (1,)), ((), ())), preferred_element_type=jnp.float32
        )
        out_ref[block] = both[:digits] + both[digits:]


def difference(weights, codebook, assign):
    return pl.pallas_call(
        difference_kernel,
        out_shape=jax.ShapeDtypeStruct(weights.shape, jnp.float32),
        in_specs=[VMEM] * 3,
        out_specs=VMEM,
        name="difference",
    )(weights, codebook, assign)


def local_mass(errors, assign, code_count):
    rows, width = errors.shape
    digits = code_count // RADIX
    out = pl.pallas_call(
        mass_kernel,
        out_shape=jax.ShapeDtypeStruct((width // LANES, digits, RADIX), jnp.float32),
        in_specs=[VMEM] * 2,
        out_specs=VMEM,
        scratch_shapes=[
            pltpu.VMEM((2 * digits, rows * LANES), jnp.bfloat16),
            pltpu.VMEM((RADIX, rows * LANES), jnp.bfloat16),
        ],
        name="mass",
    )(errors, assign)
    return out.reshape(width // LANES, code_count)


def from_root(value, axis, source):
    kept = jnp.where(lax.axis_index(axis) == source, value, 0).astype(value.dtype)
    return lax.psum(kept, axis)


def local(weights, codebook, assign, chol_upper, inv_blocks):
    block_size = inv_blocks.shape[2]
    local_blocks = inv_blocks.shape[1]
    local_width = weights.shape[2]
    code_count = codebook.shape[3]
    column_rank = lax.axis_index("col")
    block_total = local_blocks * lax.axis_size("col")
    offset_weights = difference(weights[0], codebook[0], assign[0])[None]
    column_ids = column_rank * local_width + jnp.arange(local_width, dtype=jnp.int32)
    stacked = lax.all_gather(chol_upper, "row", axis=1, tiled=True)

    def panel_of(number):
        return lax.dynamic_slice_in_dim(stacked, number * block_size, block_size, 1)

    def own_block(current, number):
        return lax.dynamic_slice_in_dim(current, number % local_blocks * block_size, block_size, 2)

    def block_error(current_block, number):
        owner_rank = number // local_blocks
        inverse = lax.dynamic_index_in_dim(inv_blocks, number % local_blocks, 1, keepdims=False)

        def compute():
            return jnp.einsum(
                "xrc,xcd->xrd", current_block, inverse, precision=lax.Precision.HIGHEST
            )

        def nothing():
            return jnp.zeros(current_block.shape, jnp.float32)

        computed = lax.cond(owner_rank == column_rank, compute, nothing)
        return from_root(computed, "col", owner_rank)

    def propagate(current, error_block, panel_rows, number, targets):
        beyond = targets >= (number + 1) * block_size
        masked = jnp.where(beyond[None, None, :], panel_rows, 0.0)
        return current - jnp.einsum(
            "xrc,xcd->xrd", error_block, masked, precision=lax.Precision.HIGHEST
        )

    def record(errors, error_block, number):
        owner_rank = number // local_blocks
        offset = number % local_blocks * block_size
        previous = lax.dynamic_slice_in_dim(errors, offset, block_size, 2)
        chosen = jnp.where(owner_rank == column_rank, error_block, previous)
        return lax.dynamic_update_slice_in_dim(errors, chosen, offset, 2)

    blank = jnp.zeros(weights.shape, jnp.float32)

    def advance(number, state_pair):
        current, errors = state_pair
        error_block = block_error(own_block(current, number), number)
        errors = record(errors, error_block, number)
        current = propagate(current, error_block, panel_of(number), number, column_ids)
        return (current, errors)

    current, errors = lax.fori_loop(0, block_total, advance, (offset_weights, blank))
    row_loss = lax.psum(jnp.sum(errors * errors, axis=2), "col")
    mass = local_mass(errors[0], assign[0], code_count)[None]
    codeword_mass = lax.psum(mass, "row")
    return (errors, row_loss, codeword_mass)


def solution(mesh):
    return jax.shard_map(
        local,
        mesh=mesh,
        in_specs=(
            P("ea", "row", "col"),
            P("ea", "col", None, None),
            P("ea", "row", "col"),
            P("ea", "row", "col"),
            P("ea", "col", None, None),
        ),
        out_specs=(P("ea", "row", "col"), P("ea", "row"), P("ea", "col", None)),
        check_vma=False,
    )
```

```python
import functools
import jax
import jax.numpy as jnp
from jax import lax
from jax.experimental import pallas as pl
from jax.experimental.pallas import tpu as pltpu
from jax.sharding import PartitionSpec as P

LANES = 128
RADIX = 16
VMEM = pl.BlockSpec(memory_space=pltpu.VMEM)


def params(flops=0, nbytes=0, limit=24):
    return dict(
        compiler_params=pltpu.CompilerParams(vmem_limit_bytes=limit * 2**20),
        cost_estimate=pl.CostEstimate(flops=flops, bytes_accessed=nbytes, transcendentals=0),
    )


def lane_take(values, index):
    return jnp.take_along_axis(values, index, axis=1, mode="promise_in_bounds")


def expanded_codes(codes, half, rows):
    lane = lax.broadcasted_iota(jnp.int32, (rows, LANES), 1)
    return lane_take(codes, half * (LANES // 2) + lane // 2)


def difference_kernel(weights_ref, codebook_ref, assign_ref, *out_refs):
    span = out_refs[0].shape[1]
    rows = weights_ref.shape[0]
    blocks, _, code_count = codebook_ref.shape
    odd = lax.broadcasted_iota(jnp.int32, (rows, LANES), 1) % 2 == 1
    for block in range(blocks):
        lanes = pl.ds(block * LANES, LANES)
        pairs = assign_ref[:, pl.ds(block // 2 * LANES, LANES)]
        code = expanded_codes(pairs, block % 2, rows)
        low = code % LANES
        page = code // LANES
        found = jnp.zeros((rows, LANES), jnp.float32)
        for part in range(code_count // LANES):
            page_lanes = pl.ds(part * LANES, LANES)
            picked = [
                lane_take(jnp.broadcast_to(codebook_ref[block, k : k + 1, page_lanes], (rows, LANES)), low)
                for k in range(2)
            ]
            found = jnp.where(page == part, jnp.where(odd, picked[1], picked[0]), found)
        place = block * LANES
        out_refs[place // span][:, pl.ds(place % span, LANES)] = weights_ref[:, lanes] - found


def mass_kernel(errors_ref, assign_ref, out_ref, left, right):
    rows = errors_ref.shape[0]
    blocks = out_ref.shape[0]
    digits = out_ref.shape[1]
    for block in range(blocks):
        err = errors_ref[:, pl.ds(block * LANES, LANES)]
        value = err * err
        upper = value.astype(jnp.bfloat16).astype(jnp.float32)
        lower = value - upper
        code = expanded_codes(assign_ref[:, pl.ds(block // 2 * LANES, LANES)], block % 2, rows)
        high = code // RADIX
        low = code % RADIX
        digit = lax.broadcasted_iota(jnp.int32, (digits, LANES), 0)
        digit_low = lax.broadcasted_iota(jnp.int32, (RADIX, LANES), 0)
        for row in range(rows):
            one = slice(row, row + 1)
            lanes = pl.ds(row * LANES, LANES)
            hit = jnp.broadcast_to(high[one], (digits, LANES)) == digit
            left[0:digits, lanes] = jnp.where(hit, jnp.broadcast_to(upper[one], hit.shape), 0.0).astype(jnp.bfloat16)
            left[digits:, lanes] = jnp.where(hit, jnp.broadcast_to(lower[one], hit.shape), 0.0).astype(jnp.bfloat16)
            match = jnp.broadcast_to(low[one], (RADIX, LANES)) == digit_low
            right[:, lanes] = jnp.where(match, 1.0, 0.0).astype(jnp.bfloat16)
        both = lax.dot_general(
            left[...], right[...], (((1,), (1,)), ((), ())), preferred_element_type=jnp.float32
        )
        out_ref[block] = both[:digits] + both[digits:]


def difference(weights, codebook, assign, pieces):
    rows, width = weights.shape
    return pl.pallas_call(
        difference_kernel,
        out_shape=[jax.ShapeDtypeStruct((rows, width // pieces), jnp.float32)] * pieces,
        in_specs=[VMEM] * 3,
        out_specs=[VMEM] * pieces,
        name="difference",
        **params(64 * rows * width, 12 * rows * width),
    )(weights, codebook, assign)


def local_mass(errors, assign, code_count):
    rows, width = errors.shape
    digits = code_count // RADIX
    out = pl.pallas_call(
        mass_kernel,
        out_shape=jax.ShapeDtypeStruct((width // LANES, digits, RADIX), jnp.float32),
        in_specs=[VMEM] * 2,
        out_specs=VMEM,
        scratch_shapes=[
            pltpu.VMEM((2 * digits, rows * LANES), jnp.bfloat16),
            pltpu.VMEM((RADIX, rows * LANES), jnp.bfloat16),
        ],
        name="mass",
    )(errors, assign)
    return out.reshape(width // LANES, code_count)


def halves(value):
    upper = value.astype(jnp.bfloat16)
    return upper, (value - upper.astype(jnp.float32)).astype(jnp.bfloat16)


def dot32(a, b):
    return jnp.dot(a, b, preferred_element_type=jnp.float32)


def dot_split(a, b_upper, b_lower):
    upper, lower = halves(a)
    return dot32(upper, b_upper) + (dot32(upper, b_lower) + dot32(lower, b_upper))


def factor_kernel(position_ref, chol_ref, inv_ref, *refs):
    span = chol_ref.shape[0]
    count = span // LANES
    place = position_ref[0]
    base = pl.multiple_of(place * span, LANES)
    inverse_upper, inverse_lower = refs[0], refs[1]
    work = refs[-1]
    work[...] = jnp.zeros((span, span), jnp.float32)
    for b in range(count):
        at = pl.ds(b * LANES, LANES)
        work[at, at] = inv_ref[place * count + b]
    width = LANES
    while width < span:
        for start in range(0, span, 2 * width):
            near, beyond = pl.ds(start, width), pl.ds(start + width, width)
            block = chol_ref[near, pl.ds(pl.multiple_of(base + start + width, LANES), width)]
            left = dot_split(work[near, near], *halves(block))
            work[near, beyond] = -dot_split(left, *halves(work[beyond, beyond]))
        width *= 2
    inverse_upper[...], inverse_lower[...] = halves(work[...])
    panels = refs[2:-1]
    for i in range(len(panels) // 2):
        panels[2 * i][...], panels[2 * i + 1][...] = halves(chol_ref[:, pl.ds(i * span, span)])


def factors(position, chol, inverses):
    span, width = chol.shape
    panel = jax.ShapeDtypeStruct((span, span), jnp.bfloat16)
    out = pl.pallas_call(
        factor_kernel,
        out_shape=[panel] * (2 + 2 * (width // span)),
        in_specs=[pl.BlockSpec(memory_space=pltpu.SMEM), VMEM, VMEM],
        out_specs=[VMEM] * (2 + 2 * (width // span)),
        scratch_shapes=[pltpu.VMEM((span, span), jnp.float32)],
        name="factors",
        **params(8 * span**3, 12 * span * width),
    )(position, chol, inverses)
    return tuple(out[:2]), [tuple(out[2 * i + 2 : 2 * i + 4]) for i in range(width // span)]


def solve_kernel(pieces, sums, near, *refs):
    out = refs[pieces + sums + 2 + 2 * near :]
    rest = jnp.concatenate([ref[...] for ref in refs[:pieces]], axis=0)
    for ref in refs[pieces : pieces + sums]:
        rest = rest - ref[...]
    inverse = refs[pieces + sums : pieces + sums + 2]
    err = dot_split(rest, inverse[0][...], inverse[1][...])
    out[0][...] = err
    if near:
        panel = refs[pieces + sums + 2 : pieces + sums + 4]
        out[1][...] = dot_split(err, panel[0][...], panel[1][...])


def solve(pieces, sums, inverse, panel, name):
    rows = sum(p.shape[0] for p in pieces)
    span = pieces[0].shape[1]
    near = panel is not None
    operands = [*pieces, *sums, *inverse, *(panel if near else ())]
    return pl.pallas_call(
        functools.partial(solve_kernel, len(pieces), len(sums), near),
        out_shape=[jax.ShapeDtypeStruct((rows, span), jnp.float32)] * (1 + near),
        in_specs=[VMEM] * len(operands),
        out_specs=[VMEM] * (1 + near),
        name=name,
        **params(6 * rows * span * span * (1 + near), 8 * rows * span),
    )(*operands)


def spread_kernel(inputs, *refs):
    err = jnp.concatenate([ref[...] for ref in refs[:inputs]], axis=0)
    upper, lower = halves(err)
    outs = len(refs[inputs:]) // 3
    panels, out = refs[inputs : inputs + 2 * outs], refs[inputs + 2 * outs :]
    for i in range(outs):
        out[i][...] = dot32(upper, panels[2 * i][...]) + (
            dot32(upper, panels[2 * i + 1][...]) + dot32(lower, panels[2 * i][...])
        )


def spread(errs, panels, name):
    rows = sum(e.shape[0] for e in errs)
    span = errs[0].shape[1]
    operands = [*errs, *(half for panel in panels for half in panel)]
    return pl.pallas_call(
        functools.partial(spread_kernel, len(errs)),
        out_shape=[jax.ShapeDtypeStruct((rows, span), jnp.float32)] * len(panels),
        in_specs=[VMEM] * len(operands),
        out_specs=[VMEM] * len(panels),
        name=name,
        **params(6 * rows * span * span * len(panels), 8 * rows * span),
    )(*operands)


def finish_kernel(groups, mine_ref, assign_ref, *refs):
    errors_ref, loss_ref, mass_ref, left, right = refs[-5:]
    span = refs[0].shape[1]
    at = 0
    for i, (returned, owned) in enumerate(groups):
        total = refs[at][...]
        for ref in refs[at + 1 : at + returned]:
            total = total + ref[...]
        for n, ref in enumerate(refs[at + returned : at + returned + owned]):
            total = jnp.where(mine_ref[i * owned + n] == 1, ref[...], total)
        errors_ref[:, pl.ds(i * span, span)] = total
        at += returned + owned
    squares = errors_ref[...] * errors_ref[...]
    loss_ref[...] = jnp.sum(squares, axis=1, keepdims=True)
    mass_kernel(errors_ref, assign_ref, mass_ref, left, right)


def finish(mine, assign, groups, code_count):
    rows, pairs = assign.shape
    width = 2 * pairs
    digits = code_count // RADIX
    blocks = width // LANES
    operands = [x for returned, owned in groups for x in (*returned, *owned)]
    return pl.pallas_call(
        functools.partial(finish_kernel, [(len(r), len(o)) for r, o in groups]),
        out_shape=[
            jax.ShapeDtypeStruct((rows, width), jnp.float32),
            jax.ShapeDtypeStruct((rows, 1), jnp.float32),
            jax.ShapeDtypeStruct((blocks, digits, RADIX), jnp.float32),
        ],
        in_specs=[pl.BlockSpec(memory_space=pltpu.SMEM)] + [VMEM] * (1 + len(operands)),
        out_specs=[VMEM] * 3,
        scratch_shapes=[
            pltpu.VMEM((2 * digits, rows * LANES), jnp.bfloat16),
            pltpu.VMEM((RADIX, rows * LANES), jnp.bfloat16),
        ],
        name="finish",
        **params(4 * 16 * 32 * rows * width, 8 * rows * width),
    )(mine, assign, *operands)


BATCHES = 2


def chained(weights, codebook, assign, chol_upper, inv_blocks):
    chips = lax.axis_size("row")
    z, c = lax.axis_index("row"), lax.axis_index("col")
    rows, width = weights.shape[1:]
    span = chol_upper.shape[1]
    per = width // span
    code_count = codebook.shape[3]
    assign = assign[0]

    def send(value, pairs):
        return lax.ppermute(value, ("row", "col"), [(a * 2 + b, p * 2 + q) for (a, b), (p, q) in pairs])

    def col_of(j):
        return j // per

    local = difference(weights[0], codebook[0], assign, per)
    inverse, panels = factors((z % per)[None].astype(jnp.int32), chol_upper[0], inv_blocks[0])

    arrived = {}
    for i in range(per):
        for r in range(1, chips):
            pairs = [(((per * q + i + r) % chips, q), (per * q + i, q)) for q in range(2)]
            arrived[i, r] = send(local[i], pairs)

    def rows_for(j, home):
        i, r = j % per, (home - j) % chips
        return local[i] if r == 0 else arrived[i, r]

    each = chips // BATCHES
    batches = [list(range(b * each, (b + 1) * each)) for b in range(BATCHES)]
    incoming = {(j, b): [] for j in range(chips) for b in range(BATCHES)}
    solved = {}
    for j in range(chips):
        here = col_of(j)
        later = range(j + 1, chips)
        elsewhere = [t for t in later if col_of(t) != here]
        near_here = j + 1 < chips and col_of(j + 1) == here
        moved = []
        for b, homes in enumerate(batches):
            outs = solve(
                [rows_for(j, home) for home in homes],
                incoming[j, b],
                inverse,
                panels[(j + 1) % per] if near_here else None,
                f"solve{j}{b}",
            )
            solved[j, b] = outs[0]
            if near_here:
                incoming[j + 1, b].append(send(outs[1], [((j, here), (j + 1, here))]))
            if elsewhere:
                moved.append(send(outs[0], [((j, here), (j, 1 - here))]))
            if elsewhere and not near_here:
                (product,) = spread([moved[b]], [panels[(j + 1) % per]], f"near{j}{b}")
                incoming[j + 1, b].append(send(product, [((j, 1 - here), (j + 1, 1 - here))]))
        for t in later:
            if t == j + 1:
                continue
            errs = [solved[j, b] for b in range(BATCHES)] if col_of(t) == here else moved
            for b in range(BATCHES):
                (product,) = spread([errs[b]], [panels[t % per]], f"far{j}{t}{b}")
                incoming[t, b].append(send(product, [((j, col_of(t)), (t, col_of(t)))]))

    def piece(j, home):
        b, place = home // each, home % each
        return lax.slice_in_dim(solved[j, b], place * rows, (place + 1) * rows, axis=0)

    groups, mine = [], []
    for i in range(per):
        returned = []
        for r in range(1, chips):
            targets = [(per * q + i, (per * q + i + r) % chips) for q in range(2)]
            value = jnp.where(c == 0, piece(*targets[0]), piece(*targets[1]))
            returned.append(send(value, [((j, q), (home, q)) for q, (j, home) in enumerate(targets)]))
        owned = [piece(per * q + i, per * q + i) for q in range(2)]
        mine += [(c == q) & (z == per * q + i) for q in range(2)]
        groups.append((returned, owned))
    errors, loss, mass = finish(jnp.stack(mine).astype(jnp.int32), assign, groups, code_count)
    loss = loss[:, 0]
    loss = loss + lax.ppermute(loss, "col", [(0, 1), (1, 0)])
    mass = mass.reshape(-1, code_count)
    step = 1
    while step < chips:
        mass = mass + lax.ppermute(mass, "row", [(n, n ^ step) for n in range(chips)])
        step *= 2
    return errors[None], loss[None], mass[None]


def from_root(value, axis, source):
    kept = jnp.where(lax.axis_index(axis) == source, value, 0).astype(value.dtype)
    return lax.psum(kept, axis)


def general(weights, codebook, assign, chol_upper, inv_blocks):
    block_size = inv_blocks.shape[2]
    local_blocks = inv_blocks.shape[1]
    local_width = weights.shape[2]
    code_count = codebook.shape[3]
    column_rank = lax.axis_index("col")
    block_total = local_blocks * lax.axis_size("col")
    offset_weights = difference(weights[0], codebook[0], assign[0], 1)[0][None]
    column_ids = column_rank * local_width + jnp.arange(local_width, dtype=jnp.int32)
    stacked = lax.all_gather(chol_upper, "row", axis=1, tiled=True)

    def panel_of(number):
        return lax.dynamic_slice_in_dim(stacked, number * block_size, block_size, 1)

    def own_block(current, number):
        return lax.dynamic_slice_in_dim(current, number % local_blocks * block_size, block_size, 2)

    def block_error(current_block, number):
        owner_rank = number // local_blocks
        inverse = lax.dynamic_index_in_dim(inv_blocks, number % local_blocks, 1, keepdims=False)

        def compute():
            return jnp.einsum(
                "xrc,xcd->xrd", current_block, inverse, precision=lax.Precision.HIGHEST
            )

        def nothing():
            return jnp.zeros(current_block.shape, jnp.float32)

        computed = lax.cond(owner_rank == column_rank, compute, nothing)
        return from_root(computed, "col", owner_rank)

    def propagate(current, error_block, panel_rows, number, targets):
        beyond = targets >= (number + 1) * block_size
        masked = jnp.where(beyond[None, None, :], panel_rows, 0.0)
        return current - jnp.einsum(
            "xrc,xcd->xrd", error_block, masked, precision=lax.Precision.HIGHEST
        )

    def record(errors, error_block, number):
        owner_rank = number // local_blocks
        offset = number % local_blocks * block_size
        previous = lax.dynamic_slice_in_dim(errors, offset, block_size, 2)
        chosen = jnp.where(owner_rank == column_rank, error_block, previous)
        return lax.dynamic_update_slice_in_dim(errors, chosen, offset, 2)

    blank = jnp.zeros(weights.shape, jnp.float32)

    def advance(number, state_pair):
        current, errors = state_pair
        error_block = block_error(own_block(current, number), number)
        errors = record(errors, error_block, number)
        current = propagate(current, error_block, panel_of(number), number, column_ids)
        return (current, errors)

    current, errors = lax.fori_loop(0, block_total, advance, (offset_weights, blank))
    row_loss = lax.psum(jnp.sum(errors * errors, axis=2), "col")
    mass = local_mass(errors[0], assign[0], code_count)[None]
    codeword_mass = lax.psum(mass, "row")
    return (errors, row_loss, codeword_mass)


def local(weights, codebook, assign, chol_upper, inv_blocks):
    count = chol_upper.shape[1] // LANES
    chips = lax.axis_size("row")
    if (
        lax.axis_size("col") == 2
        and chol_upper.shape[1] == count * LANES
        and count & (count - 1) == 0
        and chips & (chips - 1) == 0
        and chips % BATCHES == 0
    ):
        return chained(weights, codebook, assign, chol_upper, inv_blocks)
    return general(weights, codebook, assign, chol_upper, inv_blocks)


def solution(mesh):
    return jax.shard_map(
        local,
        mesh=mesh,
        in_specs=(
            P("ea", "row", "col"),
            P("ea", "col", None, None),
            P("ea", "row", "col"),
            P("ea", "row", "col"),
            P("ea", "col", None, None),
        ),
        out_specs=(P("ea", "row", "col"), P("ea", "row"), P("ea", "col", None)),
        check_vma=False,
    )
```

```python
import functools
import jax
import jax.numpy as jnp
from jax import lax
from jax.experimental import pallas as pl
from jax.experimental.pallas import tpu as pltpu
from jax.sharding import PartitionSpec as P

LANES = 128
RADIX = 16
VMEM = pl.BlockSpec(memory_space=pltpu.VMEM)


def params(flops=0, nbytes=0, limit=16):
    return dict(
        compiler_params=pltpu.CompilerParams(vmem_limit_bytes=limit * 2**20),
        cost_estimate=pl.CostEstimate(flops=flops, bytes_accessed=nbytes, transcendentals=0),
    )


def lane_take(values, index):
    return jnp.take_along_axis(values, index, axis=1, mode="promise_in_bounds")


def expanded_codes(codes, half, rows):
    lane = lax.broadcasted_iota(jnp.int32, (rows, LANES), 1)
    return lane_take(codes, half * (LANES // 2) + lane // 2)


def difference_kernel(weights_hbm, codebook_hbm, assign_hbm, *refs):
    weights_ref, codebook_ref, assign_ref, sems = refs[-4:]
    out_refs = refs[:-4]
    copies = [
        pltpu.make_async_copy(src, dst, sems.at[n])
        for n, (src, dst) in enumerate(
            [(codebook_hbm, codebook_ref), (assign_hbm, assign_ref), (weights_hbm, weights_ref)]
        )
    ]
    for copy in copies:
        copy.start()
    for copy in copies:
        copy.wait()
    span = out_refs[0].shape[1]
    rows = weights_ref.shape[0]
    blocks, _, code_count = codebook_ref.shape
    odd = lax.broadcasted_iota(jnp.int32, (rows, LANES), 1) % 2 == 1
    for block in range(blocks):
        lanes = pl.ds(block * LANES, LANES)
        pairs = assign_ref[:, pl.ds(block // 2 * LANES, LANES)]
        code = expanded_codes(pairs, block % 2, rows)
        low = code % LANES
        page = code // LANES
        found = jnp.zeros((rows, LANES), jnp.float32)
        for part in range(code_count // LANES):
            page_lanes = pl.ds(part * LANES, LANES)
            picked = [
                lane_take(jnp.broadcast_to(codebook_ref[block, k : k + 1, page_lanes], (rows, LANES)), low)
                for k in range(2)
            ]
            found = jnp.where(page == part, jnp.where(odd, picked[1], picked[0]), found)
        place = block * LANES
        out_refs[place // span][:, pl.ds(place % span, LANES)] = weights_ref[:, lanes] - found


def mass_kernel(errors_ref, assign_ref, out_ref, left, right, first=0):
    rows = errors_ref.shape[0]
    blocks = out_ref.shape[0]
    digits = out_ref.shape[1]
    for block in range(blocks):
        err = errors_ref[:, pl.ds(block * LANES, LANES)]
        value = err * err
        upper = value.astype(jnp.bfloat16).astype(jnp.float32)
        lower = value - upper
        number = first + block
        code = expanded_codes(assign_ref[:, pl.ds(number // 2 * LANES, LANES)], number % 2, rows)
        high = code // RADIX
        low = code % RADIX
        digit = lax.broadcasted_iota(jnp.int32, (digits, LANES), 0)
        digit_low = lax.broadcasted_iota(jnp.int32, (RADIX, LANES), 0)
        for row in range(rows):
            one = slice(row, row + 1)
            lanes = pl.ds(row * LANES, LANES)
            hit = jnp.broadcast_to(high[one], (digits, LANES)) == digit
            left[0:digits, lanes] = jnp.where(hit, jnp.broadcast_to(upper[one], hit.shape), 0.0).astype(jnp.bfloat16)
            left[digits:, lanes] = jnp.where(hit, jnp.broadcast_to(lower[one], hit.shape), 0.0).astype(jnp.bfloat16)
            match = jnp.broadcast_to(low[one], (RADIX, LANES)) == digit_low
            right[:, lanes] = jnp.where(match, 1.0, 0.0).astype(jnp.bfloat16)
        both = lax.dot_general(
            left[...], right[...], (((1,), (1,)), ((), ())), preferred_element_type=jnp.float32
        )
        out_ref[block] = both[:digits] + both[digits:]


def difference(weights, codebook, assign, pieces):
    rows, width = weights.shape
    return pl.pallas_call(
        difference_kernel,
        out_shape=[jax.ShapeDtypeStruct((rows, width // pieces), jnp.float32)] * pieces,
        in_specs=[pl.BlockSpec(memory_space=pltpu.HBM)] * 3,
        out_specs=[VMEM] * pieces,
        scratch_shapes=[
            pltpu.VMEM(weights.shape, weights.dtype),
            pltpu.VMEM(codebook.shape, codebook.dtype),
            pltpu.VMEM(assign.shape, assign.dtype),
            pltpu.SemaphoreType.DMA((3,)),
        ],
        name="difference",
        **params(64 * rows * width, 12 * rows * width, 62),
    )(weights, codebook, assign)


def local_mass(errors, assign, code_count):
    rows, width = errors.shape
    digits = code_count // RADIX
    out = pl.pallas_call(
        mass_kernel,
        out_shape=jax.ShapeDtypeStruct((width // LANES, digits, RADIX), jnp.float32),
        in_specs=[VMEM] * 2,
        out_specs=VMEM,
        scratch_shapes=[
            pltpu.VMEM((2 * digits, rows * LANES), jnp.bfloat16),
            pltpu.VMEM((RADIX, rows * LANES), jnp.bfloat16),
        ],
        name="mass",
    )(errors, assign)
    return out.reshape(width // LANES, code_count)


def halves(value):
    upper = value.astype(jnp.bfloat16)
    return upper, (value - upper.astype(jnp.float32)).astype(jnp.bfloat16)


def dot32(a, b):
    return jnp.dot(a, b, preferred_element_type=jnp.float32)


def dot_split(a, b_upper, b_lower):
    upper, lower = halves(a)
    return dot32(upper, b_upper) + (dot32(upper, b_lower) + dot32(lower, b_upper))


def factor_kernel(first_chip, last_chip, chips, own_chol, other_chol, own_inv, other_inv, *refs):
    out, (work, blocks, sems) = refs[:-3], refs[-3:]
    span = own_chol.shape[0]
    count = span // LANES
    per = own_chol.shape[1] // span
    chip, mine = lax.axis_index("row"), lax.axis_index("col")
    place, wanted = lax.rem(chip, per), lax.div(chip, per)
    diagonal = pl.ds(pl.multiple_of(place * span, span), span)
    inv_at = pl.ds(place * count, count)

    def transfer(source, target, sem, chosen):
        def start():
            for src, condition in zip(source, (chosen, jnp.logical_not(chosen))):
                @pl.when(condition)
                def _():
                    pltpu.make_async_copy(src, target, sem).start()

        return start, pltpu.make_async_copy(source[0], target, sem).wait

    @pl.when((chip >= first_chip) & (chip <= last_chip))
    def _():
        here = mine == wanted
        first = [
            transfer((own_inv.at[inv_at], other_inv.at[inv_at]), blocks, sems.at[0], here),
            transfer((own_chol.at[:, diagonal], other_chol.at[:, diagonal]), work.at[0], sems.at[1], here),
        ]
        panels = {}
        for t in range(first_chip + 1, chips):
            columns = pl.ds(t % per * span, span)
            source = (own_chol.at[:, columns], other_chol.at[:, columns])
            panels[t] = transfer(source, work.at[t], sems.at[t + 1], mine == t // per)
        for start, _ in first:
            start()
        for t, (start, _) in panels.items():
            pl.when(t > chip)(start)
        for _, wait in first:
            wait()
        inverse = work.at[chips]
        inverse[...] = jnp.zeros((span, span), jnp.float32)
        for b in range(count):
            at = pl.ds(b * LANES, LANES)
            inverse[at, at] = blocks[b]
        width = LANES
        while width < span:
            for begin in range(0, span, 2 * width):
                near, beyond = pl.ds(begin, width), pl.ds(begin + width, width)
                left = dot_split(inverse[near, near], *halves(work[0, near, beyond]))
                inverse[near, beyond] = -dot_split(left, *halves(inverse[beyond, beyond]))
            width *= 2
        out[0][0], out[0][1] = halves(inverse[...])
        for t, (_, wait) in panels.items():
            @pl.when(t > chip)
            def _():
                wait()
                out[t][0], out[t][1] = halves(work[t])


def factors(first_chip, last_chip, chips, chol, other_chol, inverses, other_inverses):
    span, width = chol.shape
    count = span // LANES
    return pl.pallas_call(
        functools.partial(factor_kernel, first_chip, last_chip, chips),
        out_shape=[jax.ShapeDtypeStruct((2, span, span), jnp.bfloat16)] * chips,
        in_specs=[pl.BlockSpec(memory_space=pltpu.HBM)] * 4,
        out_specs=[VMEM] * chips,
        scratch_shapes=[
            pltpu.VMEM((chips + 1, span, span), jnp.float32),
            pltpu.VMEM((count, LANES, LANES), jnp.float32),
            pltpu.SemaphoreType.DMA((chips + 1,)),
        ],
        **params(8 * span**3, 24 * span * width, 16),
    )(chol, other_chol, inverses, other_inverses)


def solve_kernel(pieces, offsets, bases, panels, *refs):
    inputs = pieces + len(offsets) + len(bases)
    rest = jnp.concatenate([ref[...] for ref in refs[:pieces]], axis=0)
    factor = refs[inputs : inputs + 1 + panels]
    out = refs[inputs + 1 + panels :]
    span = rest.shape[1]
    for ref, at in zip(refs[pieces:], offsets):
        rest = rest - ref[:, pl.ds(at, span)]
    err = dot_split(rest, factor[0][0], factor[0][1])
    out[0][...] = err
    upper, lower = halves(err)
    for n in range(panels):
        panel = factor[n + 1]
        product = dot32(upper, panel[0]) + (dot32(upper, panel[1]) + dot32(lower, panel[0]))
        for which, at in bases:
            if which[0] == n:
                product = product + refs[which[1]][:, pl.ds(at, span)]
        out[1][:, pl.ds(n * span, span)] = product


def solve(pieces, sums, bases, factor, panels):
    rows = sum(p.shape[0] for p in pieces)
    span = pieces[0].shape[1]
    operands = [*pieces, *(array for array, _ in sums)]
    marks = []
    for n, (array, at) in bases:
        marks.append(((n, len(operands)), at))
        operands.append(array)
    operands += [factor[t] for t in (0, *panels)]
    shapes = [jax.ShapeDtypeStruct((rows, span), jnp.float32)]
    if panels:
        shapes.append(jax.ShapeDtypeStruct((rows, len(panels) * span), jnp.float32))
    return pl.pallas_call(
        functools.partial(solve_kernel, len(pieces), [at for _, at in sums], marks, len(panels)),
        out_shape=shapes,
        in_specs=[VMEM] * len(operands),
        out_specs=[VMEM] * len(shapes),
        **params(6 * rows * span * span * (1 + len(panels)), 8 * rows * span),
    )(*operands)


def spread_kernel(err_ref, panel, *refs):
    total = dot_split(err_ref[...], panel[0], panel[1])
    for ref in refs[:-1]:
        total = total + ref[...]
    refs[-1][...] = total


def spread(err, panel, bases):
    rows, span = err.shape
    return pl.pallas_call(
        spread_kernel,
        out_shape=jax.ShapeDtypeStruct((rows, span), jnp.float32),
        in_specs=[VMEM] * (2 + len(bases)),
        out_specs=VMEM,
        **params(6 * rows * span * span, 8 * rows * span),
    )(err, panel, *bases)


def finish_kernel(returned, first, assign_ref, *refs):
    total = refs[0][...]
    for ref in refs[1:returned]:
        total = total + ref[...]
    left, right = refs[-2:]
    errors_ref, loss_ref, mass_ref = refs[-5:-2]
    errors_ref[...] = total
    loss_ref[...] = jnp.sum(total * total, axis=1, keepdims=True)
    mass_kernel(errors_ref, assign_ref, mass_ref, left, right, first)


def finish(assign, returned, first, code_count):
    rows, span = returned[0].shape
    digits = code_count // RADIX
    return pl.pallas_call(
        functools.partial(finish_kernel, len(returned), first),
        out_shape=[
            jax.ShapeDtypeStruct((rows, span), jnp.float32),
            jax.ShapeDtypeStruct((rows, 1), jnp.float32),
            jax.ShapeDtypeStruct((span // LANES, digits, RADIX), jnp.float32),
        ],
        in_specs=[VMEM] * (1 + len(returned)),
        out_specs=[VMEM] * 3,
        scratch_shapes=[
            pltpu.VMEM((2 * digits, rows * LANES), jnp.bfloat16),
            pltpu.VMEM((RADIX, rows * LANES), jnp.bfloat16),
        ],
        **params(4 * 16 * 32 * rows * span, 8 * rows * span),
    )(assign, *returned)


def chained(weights, codebook, assign, chol_upper, inv_blocks):
    chips = lax.axis_size("row")
    z = lax.axis_index("row")
    rows, width = weights.shape[1:]
    span = chol_upper.shape[1]
    per = width // span
    each = chips // 2
    code_count = codebook.shape[3]
    assign = assign[0]

    def send(value, pairs):
        return lax.ppermute(value, ("row", "col"), [(a * 2 + b, p * 2 + q) for (a, b), (p, q) in pairs])

    def swapped(value):
        return send(value, [((n, q), (n, 1 - q)) for n in range(chips) for q in range(2)])

    def forward(value, j, t):
        return send(value, [((j, n), (t, n)) for n in range(2)])

    def routes(i, part):
        return [((n * each + part, q), (q * per + i, n)) for q in range(2) for n in range(2)]

    other_chol = swapped(chol_upper[0])
    other_inv = swapped(inv_blocks[0])
    local = difference(weights[0], codebook[0], assign, per)
    arrived = {
        (i, part): send(local[i], routes(i, part)) for i in range(per) for part in range(each)
    }
    halves_held = (chol_upper[0], other_chol, inv_blocks[0], other_inv)
    factor = factors(0, chips - 1, chips, *halves_held)

    incoming = {}
    solved = {}
    for j in range(chips):
        first = list(range(j + 1, min(chips, j + 2 + (j == 0))))
        outs = solve(
            [arrived[j % per, part] for part in range(each)],
            [incoming[j]] if j in incoming else [],
            [(n, incoming[t]) for n, t in enumerate(first) if t in incoming],
            factor,
            first,
        )
        solved[j] = outs[0]
        sent = {}
        if first:
            moved = forward(outs[1], j, j + 1)
            sent = {t: (moved, n * span) for n, t in enumerate(first)}
        for t in range(j + 1 + len(first), chips):
            product = spread(outs[0], factor[t], [incoming[t][0]] if t in incoming else [])
            sent[t] = (forward(product, j, j + 1), 0)
        incoming = sent

    errors, losses, masses = [], [], []
    for i in range(per):
        chosen = jnp.where(z == i, solved[i], solved[per + i])
        returned = []
        for part in range(each):
            value = lax.slice_in_dim(chosen, part * rows, (part + 1) * rows, axis=0)
            returned.append(send(value, [(b, a) for a, b in routes(i, part)]))
        total, loss, mass = finish(assign, returned, i * span // LANES, code_count)
        errors.append(total)
        losses.append(loss)
        masses.append(mass)
    loss = sum(losses[1:], losses[0])[:, 0]
    loss = loss + swapped(loss)
    mass = jnp.concatenate(masses, axis=0).reshape(-1, code_count)
    step = 1
    while step < chips:
        pairs = [((n, q), (n ^ step, q)) for n in range(chips) for q in range(2)]
        mass = mass + send(mass, pairs)
        step *= 2
    return jnp.concatenate(errors, axis=1)[None], loss[None], mass[None]


def from_root(value, axis, source):
    kept = jnp.where(lax.axis_index(axis) == source, value, 0).astype(value.dtype)
    return lax.psum(kept, axis)


def general(weights, codebook, assign, chol_upper, inv_blocks):
    block_size = inv_blocks.shape[2]
    local_blocks = inv_blocks.shape[1]
    local_width = weights.shape[2]
    code_count = codebook.shape[3]
    column_rank = lax.axis_index("col")
    block_total = local_blocks * lax.axis_size("col")
    offset_weights = difference(weights[0], codebook[0], assign[0], 1)[0][None]
    column_ids = column_rank * local_width + jnp.arange(local_width, dtype=jnp.int32)
    stacked = lax.all_gather(chol_upper, "row", axis=1, tiled=True)

    def panel_of(number):
        return lax.dynamic_slice_in_dim(stacked, number * block_size, block_size, 1)

    def own_block(current, number):
        return lax.dynamic_slice_in_dim(current, number % local_blocks * block_size, block_size, 2)

    def block_error(current_block, number):
        owner_rank = number // local_blocks
        inverse = lax.dynamic_index_in_dim(inv_blocks, number % local_blocks, 1, keepdims=False)

        def compute():
            return jnp.einsum(
                "xrc,xcd->xrd", current_block, inverse, precision=lax.Precision.HIGHEST
            )

        def nothing():
            return jnp.zeros(current_block.shape, jnp.float32)

        computed = lax.cond(owner_rank == column_rank, compute, nothing)
        return from_root(computed, "col", owner_rank)

    def propagate(current, error_block, panel_rows, number, targets):
        beyond = targets >= (number + 1) * block_size
        masked = jnp.where(beyond[None, None, :], panel_rows, 0.0)
        return current - jnp.einsum(
            "xrc,xcd->xrd", error_block, masked, precision=lax.Precision.HIGHEST
        )

    def record(errors, error_block, number):
        owner_rank = number // local_blocks
        offset = number % local_blocks * block_size
        previous = lax.dynamic_slice_in_dim(errors, offset, block_size, 2)
        chosen = jnp.where(owner_rank == column_rank, error_block, previous)
        return lax.dynamic_update_slice_in_dim(errors, chosen, offset, 2)

    blank = jnp.zeros(weights.shape, jnp.float32)

    def advance(number, state_pair):
        current, errors = state_pair
        error_block = block_error(own_block(current, number), number)
        errors = record(errors, error_block, number)
        current = propagate(current, error_block, panel_of(number), number, column_ids)
        return (current, errors)

    _, errors = lax.fori_loop(0, block_total, advance, (offset_weights, blank))
    row_loss = lax.psum(jnp.sum(errors * errors, axis=2), "col")
    mass = local_mass(errors[0], assign[0], code_count)[None]
    codeword_mass = lax.psum(mass, "row")
    return (errors, row_loss, codeword_mass)


def local(weights, codebook, assign, chol_upper, inv_blocks):
    count = chol_upper.shape[1] // LANES
    chips = lax.axis_size("row")
    if (
        lax.axis_size("col") == 2
        and chol_upper.shape[1] == count * LANES
        and count & (count - 1) == 0
        and chips & (chips - 1) == 0
        and chips > 1
        and chips * chol_upper.shape[1] == 2 * weights.shape[2]
    ):
        return chained(weights, codebook, assign, chol_upper, inv_blocks)
    return general(weights, codebook, assign, chol_upper, inv_blocks)


def solution(mesh):
    return jax.shard_map(
        local,
        mesh=mesh,
        in_specs=(
            P("ea", "row", "col"),
            P("ea", "col", None, None),
            P("ea", "row", "col"),
            P("ea", "row", "col"),
            P("ea", "col", None, None),
        ),
        out_specs=(P("ea", "row", "col"), P("ea", "row"), P("ea", "col", None)),
        check_vma=False,
    )
```

```python
import functools
import jax
import jax.numpy as jnp
from jax import lax
from jax.experimental import pallas as pl
from jax.experimental.pallas import tpu as pltpu
from jax.sharding import PartitionSpec as P

LANES = 128
RADIX = 16
VMEM = pl.BlockSpec(memory_space=pltpu.VMEM)


def params(flops=0, nbytes=0, limit=16):
    return dict(
        compiler_params=pltpu.CompilerParams(vmem_limit_bytes=limit * 2**20),
        cost_estimate=pl.CostEstimate(flops=flops, bytes_accessed=nbytes, transcendentals=0),
    )


def lane_take(values, index):
    return jnp.take_along_axis(values, index, axis=1, mode="promise_in_bounds")


def expanded_codes(codes, half, rows):
    lane = lax.broadcasted_iota(jnp.int32, (rows, LANES), 1)
    return lane_take(codes, half * (LANES // 2) + lane // 2)


def difference_kernel(weights_hbm, codebook_hbm, assign_hbm, *refs):
    weights_ref, codebook_ref, assign_ref, sems = refs[-4:]
    out_refs = refs[:-4]
    copies = [
        pltpu.make_async_copy(src, dst, sems.at[n])
        for n, (src, dst) in enumerate(
            [(codebook_hbm, codebook_ref), (assign_hbm, assign_ref), (weights_hbm, weights_ref)]
        )
    ]
    for copy in copies:
        copy.start()
    for copy in copies[:2]:
        copy.wait()
    span = out_refs[0].shape[1]
    rows = weights_ref.shape[0]
    blocks, _, code_count = codebook_ref.shape
    odd = lax.broadcasted_iota(jnp.int32, (rows, LANES), 1) % 2 == 1
    for block in range(blocks):
        lanes = pl.ds(block * LANES, LANES)
        pairs = assign_ref[:, pl.ds(block // 2 * LANES, LANES)]
        code = expanded_codes(pairs, block % 2, rows)
        low = code % LANES
        page = code // LANES
        found = jnp.zeros((rows, LANES), jnp.float32)
        for part in range(code_count // LANES):
            page_lanes = pl.ds(part * LANES, LANES)
            picked = [
                lane_take(jnp.broadcast_to(codebook_ref[block, k : k + 1, page_lanes], (rows, LANES)), low)
                for k in range(2)
            ]
            found = jnp.where(page == part, jnp.where(odd, picked[1], picked[0]), found)
        if block == 0:
            copies[2].wait()
        place = block * LANES
        out_refs[place // span][:, pl.ds(place % span, LANES)] = weights_ref[:, lanes] - found


def mass_kernel(errors_ref, assign_ref, out_ref, left, right, first=0):
    rows = errors_ref.shape[0]
    blocks = out_ref.shape[0]
    digits = out_ref.shape[1]
    for block in range(blocks):
        err = errors_ref[:, pl.ds(block * LANES, LANES)]
        value = err * err
        upper = value.astype(jnp.bfloat16).astype(jnp.float32)
        lower = value - upper
        number = first + block
        code = expanded_codes(assign_ref[:, pl.ds(number // 2 * LANES, LANES)], number % 2, rows)
        high = code // RADIX
        low = code % RADIX
        digit = lax.broadcasted_iota(jnp.int32, (digits, LANES), 0)
        digit_low = lax.broadcasted_iota(jnp.int32, (RADIX, LANES), 0)
        for row in range(rows):
            one = slice(row, row + 1)
            lanes = pl.ds(row * LANES, LANES)
            hit = jnp.broadcast_to(high[one], (digits, LANES)) == digit
            left[0:digits, lanes] = jnp.where(hit, jnp.broadcast_to(upper[one], hit.shape), 0.0).astype(jnp.bfloat16)
            left[digits:, lanes] = jnp.where(hit, jnp.broadcast_to(lower[one], hit.shape), 0.0).astype(jnp.bfloat16)
            match = jnp.broadcast_to(low[one], (RADIX, LANES)) == digit_low
            right[:, lanes] = jnp.where(match, 1.0, 0.0).astype(jnp.bfloat16)
        both = lax.dot_general(
            left[...], right[...], (((1,), (1,)), ((), ())), preferred_element_type=jnp.float32
        )
        out_ref[block] = both[:digits] + both[digits:]


def difference(weights, codebook, assign, pieces):
    rows, width = weights.shape
    return pl.pallas_call(
        difference_kernel,
        out_shape=[jax.ShapeDtypeStruct((rows, width // pieces), jnp.float32)] * pieces,
        in_specs=[pl.BlockSpec(memory_space=pltpu.HBM)] * 3,
        out_specs=[VMEM] * pieces,
        scratch_shapes=[
            pltpu.VMEM(weights.shape, weights.dtype),
            pltpu.VMEM(codebook.shape, codebook.dtype),
            pltpu.VMEM(assign.shape, assign.dtype),
            pltpu.SemaphoreType.DMA((3,)),
        ],
        name="difference",
        **params(64 * rows * width, 12 * rows * width, 62),
    )(weights, codebook, assign)


def local_mass(errors, assign, code_count):
    rows, width = errors.shape
    digits = code_count // RADIX
    out = pl.pallas_call(
        mass_kernel,
        out_shape=jax.ShapeDtypeStruct((width // LANES, digits, RADIX), jnp.float32),
        in_specs=[VMEM] * 2,
        out_specs=VMEM,
        scratch_shapes=[
            pltpu.VMEM((2 * digits, rows * LANES), jnp.bfloat16),
            pltpu.VMEM((RADIX, rows * LANES), jnp.bfloat16),
        ],
        name="mass",
    )(errors, assign)
    return out.reshape(width // LANES, code_count)


def halves(value):
    upper = value.astype(jnp.bfloat16)
    return upper, (value - upper.astype(jnp.float32)).astype(jnp.bfloat16)


def dot32(a, b):
    return jnp.dot(a, b, preferred_element_type=jnp.float32)


def dot_split(a, b_upper, b_lower):
    upper, lower = halves(a)
    return dot32(upper, b_upper) + (dot32(upper, b_lower) + dot32(lower, b_upper))


def factor_kernel(first_chip, last_chip, chips, own_chol, other_chol, own_inv, other_inv, *refs):
    out, (work, blocks, sems) = refs[:-3], refs[-3:]
    span = own_chol.shape[0]
    count = span // LANES
    per = own_chol.shape[1] // span
    chip, mine = lax.axis_index("row"), lax.axis_index("col")
    place, wanted = lax.rem(chip, per), lax.div(chip, per)
    diagonal = pl.ds(pl.multiple_of(place * span, span), span)
    inv_at = pl.ds(place * count, count)

    def transfer(source, target, sem, chosen):
        def start():
            for src, condition in zip(source, (chosen, jnp.logical_not(chosen))):
                @pl.when(condition)
                def _():
                    pltpu.make_async_copy(src, target, sem).start()

        return start, pltpu.make_async_copy(source[0], target, sem).wait

    @pl.when((chip >= first_chip) & (chip <= last_chip))
    def _():
        here = mine == wanted
        first = [
            transfer((own_inv.at[inv_at], other_inv.at[inv_at]), blocks, sems.at[0], here),
            transfer((own_chol.at[:, diagonal], other_chol.at[:, diagonal]), work.at[0], sems.at[1], here),
        ]
        panels = {}
        for t in range(first_chip + 1, chips):
            columns = pl.ds(t % per * span, span)
            source = (own_chol.at[:, columns], other_chol.at[:, columns])
            panels[t] = transfer(source, work.at[t], sems.at[t + 1], mine == t // per)
        for start, _ in first:
            start()
        for t, (start, _) in panels.items():
            pl.when(t > chip)(start)
        for _, wait in first:
            wait()
        inverse = work.at[chips]
        inverse[...] = jnp.zeros((span, span), jnp.float32)
        for b in range(count):
            at = pl.ds(b * LANES, LANES)
            inverse[at, at] = blocks[b]
        width = LANES
        while width < span:
            for begin in range(0, span, 2 * width):
                near, beyond = pl.ds(begin, width), pl.ds(begin + width, width)
                left = dot_split(inverse[near, near], *halves(work[0, near, beyond]))
                inverse[near, beyond] = -dot_split(left, *halves(inverse[beyond, beyond]))
            width *= 2
        out[0][0], out[0][1] = halves(inverse[...])
        for t, (_, wait) in panels.items():
            @pl.when(t > chip)
            def _():
                wait()
                out[t][0], out[t][1] = halves(work[t])


def factors(first_chip, last_chip, chips, chol, other_chol, inverses, other_inverses):
    span, width = chol.shape
    count = span // LANES
    return pl.pallas_call(
        functools.partial(factor_kernel, first_chip, last_chip, chips),
        out_shape=[jax.ShapeDtypeStruct((2, span, span), jnp.bfloat16)] * chips,
        in_specs=[pl.BlockSpec(memory_space=pltpu.HBM)] * 4,
        out_specs=[VMEM] * chips,
        scratch_shapes=[
            pltpu.VMEM((chips + 1, span, span), jnp.float32),
            pltpu.VMEM((count, LANES, LANES), jnp.float32),
            pltpu.SemaphoreType.DMA((chips + 1,)),
        ],
        **params(8 * span**3, 24 * span * width, 16),
    )(chol, other_chol, inverses, other_inverses)


def solve_kernel(pieces, offsets, bases, panels, *refs):
    inputs = pieces + len(offsets) + len(bases)
    rest = jnp.concatenate([ref[...] for ref in refs[:pieces]], axis=0)
    factor = refs[inputs : inputs + 1 + panels]
    out = refs[inputs + 1 + panels :]
    span = rest.shape[1]
    for ref, at in zip(refs[pieces:], offsets):
        rest = rest - ref[:, pl.ds(at, span)]
    err = dot_split(rest, factor[0][0], factor[0][1])
    out[0][...] = err
    upper, lower = halves(err)
    for n in range(panels):
        panel = factor[n + 1]
        product = dot32(upper, panel[0]) + (dot32(upper, panel[1]) + dot32(lower, panel[0]))
        for which, at in bases:
            if which[0] == n:
                product = product + refs[which[1]][:, pl.ds(at, span)]
        out[1][:, pl.ds(n * span, span)] = product


def solve(pieces, sums, bases, factor, panels):
    rows = sum(p.shape[0] for p in pieces)
    span = pieces[0].shape[1]
    operands = [*pieces, *(array for array, _ in sums)]
    marks = []
    for n, (array, at) in bases:
        marks.append(((n, len(operands)), at))
        operands.append(array)
    operands += [factor[t] for t in (0, *panels)]
    shapes = [jax.ShapeDtypeStruct((rows, span), jnp.float32)]
    if panels:
        shapes.append(jax.ShapeDtypeStruct((rows, len(panels) * span), jnp.float32))
    return pl.pallas_call(
        functools.partial(solve_kernel, len(pieces), [at for _, at in sums], marks, len(panels)),
        out_shape=shapes,
        in_specs=[VMEM] * len(operands),
        out_specs=[VMEM] * len(shapes),
        **params(6 * rows * span * span * (1 + len(panels)), 8 * rows * span),
    )(*operands)


def spread_kernel(err_ref, panel, *refs):
    total = dot_split(err_ref[...], panel[0], panel[1])
    for ref in refs[:-1]:
        total = total + ref[...]
    refs[-1][...] = total


def spread(err, panel, bases):
    rows, span = err.shape
    return pl.pallas_call(
        spread_kernel,
        out_shape=jax.ShapeDtypeStruct((rows, span), jnp.float32),
        in_specs=[VMEM] * (2 + len(bases)),
        out_specs=VMEM,
        **params(6 * rows * span * span, 8 * rows * span),
    )(err, panel, *bases)


def finish_kernel(returned, first, assign_ref, *refs):
    total = refs[0][...]
    for ref in refs[1:returned]:
        total = total + ref[...]
    left, right = refs[-2:]
    errors_ref, loss_ref, mass_ref = refs[-5:-2]
    errors_ref[...] = total
    loss_ref[...] = jnp.sum(total * total, axis=1, keepdims=True)
    mass_kernel(errors_ref, assign_ref, mass_ref, left, right, first)


def finish(assign, returned, first, code_count):
    rows, span = returned[0].shape
    digits = code_count // RADIX
    return pl.pallas_call(
        functools.partial(finish_kernel, len(returned), first),
        out_shape=[
            jax.ShapeDtypeStruct((rows, span), jnp.float32),
            jax.ShapeDtypeStruct((rows, 1), jnp.float32),
            jax.ShapeDtypeStruct((span // LANES, digits, RADIX), jnp.float32),
        ],
        in_specs=[VMEM] * (1 + len(returned)),
        out_specs=[VMEM] * 3,
        scratch_shapes=[
            pltpu.VMEM((2 * digits, rows * LANES), jnp.bfloat16),
            pltpu.VMEM((RADIX, rows * LANES), jnp.bfloat16),
        ],
        **params(4 * 16 * 32 * rows * span, 8 * rows * span),
    )(assign, *returned)


def chained(weights, codebook, assign, chol_upper, inv_blocks):
    chips = lax.axis_size("row")
    z = lax.axis_index("row")
    rows, width = weights.shape[1:]
    span = chol_upper.shape[1]
    per = width // span
    each = chips // 2
    code_count = codebook.shape[3]
    assign = assign[0]

    def send(value, pairs):
        return lax.ppermute(value, ("row", "col"), [(a * 2 + b, p * 2 + q) for (a, b), (p, q) in pairs])

    def swapped(value):
        return send(value, [((n, q), (n, 1 - q)) for n in range(chips) for q in range(2)])

    def forward(value, j, t):
        return send(value, [((j, n), (t, n)) for n in range(2)])

    def routes(i, part):
        return [((n * each + part, q), (q * per + i, n)) for q in range(2) for n in range(2)]

    other_chol = swapped(chol_upper[0])
    other_inv = swapped(inv_blocks[0])
    local = difference(weights[0], codebook[0], assign, per)
    arrived = {
        (i, part): send(local[i], routes(i, part)) for i in range(per) for part in range(each)
    }
    halves_held = (chol_upper[0], other_chol, inv_blocks[0], other_inv)
    factor = factors(0, chips - 1, chips, *halves_held)

    incoming = {}
    solved = {}
    for j in range(chips):
        first = list(range(j + 1, min(chips, j + 2 + (j == 0))))
        outs = solve(
            [arrived[j % per, part] for part in range(each)],
            [incoming[j]] if j in incoming else [],
            [(n, incoming[t]) for n, t in enumerate(first) if t in incoming],
            factor,
            first,
        )
        solved[j] = outs[0]
        sent = {}
        if first:
            moved = forward(outs[1], j, j + 1)
            sent = {t: (moved, n * span) for n, t in enumerate(first)}
        for t in range(j + 1 + len(first), chips):
            product = spread(outs[0], factor[t], [incoming[t][0]] if t in incoming else [])
            sent[t] = (forward(product, j, j + 1), 0)
        incoming = sent

    errors, losses, masses = [], [], []
    for i in range(per):
        chosen = jnp.where(z == i, solved[i], solved[per + i])
        returned = []
        for part in range(each):
            value = lax.slice_in_dim(chosen, part * rows, (part + 1) * rows, axis=0)
            returned.append(send(value, [(b, a) for a, b in routes(i, part)]))
        total, loss, mass = finish(assign, returned, i * span // LANES, code_count)
        errors.append(total)
        losses.append(loss)
        masses.append(mass)
    loss = sum(losses[1:], losses[0])[:, 0]
    loss = loss + swapped(loss)
    mass = jnp.concatenate(masses, axis=0).reshape(-1, code_count)
    step = chips // 2
    while step:
        pairs = [((n, q), (n ^ step, q)) for n in range(chips) for q in range(2)]
        mass = mass + send(mass, pairs)
        step //= 2
    return jnp.concatenate(errors, axis=1)[None], loss[None], mass[None]


def from_root(value, axis, source):
    kept = jnp.where(lax.axis_index(axis) == source, value, 0).astype(value.dtype)
    return lax.psum(kept, axis)


def general(weights, codebook, assign, chol_upper, inv_blocks):
    block_size = inv_blocks.shape[2]
    local_blocks = inv_blocks.shape[1]
    local_width = weights.shape[2]
    code_count = codebook.shape[3]
    column_rank = lax.axis_index("col")
    block_total = local_blocks * lax.axis_size("col")
    offset_weights = difference(weights[0], codebook[0], assign[0], 1)[0][None]
    column_ids = column_rank * local_width + jnp.arange(local_width, dtype=jnp.int32)
    stacked = lax.all_gather(chol_upper, "row", axis=1, tiled=True)

    def panel_of(number):
        return lax.dynamic_slice_in_dim(stacked, number * block_size, block_size, 1)

    def own_block(current, number):
        return lax.dynamic_slice_in_dim(current, number % local_blocks * block_size, block_size, 2)

    def block_error(current_block, number):
        owner_rank = number // local_blocks
        inverse = lax.dynamic_index_in_dim(inv_blocks, number % local_blocks, 1, keepdims=False)

        def compute():
            return jnp.einsum(
                "xrc,xcd->xrd", current_block, inverse, precision=lax.Precision.HIGHEST
            )

        def nothing():
            return jnp.zeros(current_block.shape, jnp.float32)

        computed = lax.cond(owner_rank == column_rank, compute, nothing)
        return from_root(computed, "col", owner_rank)

    def propagate(current, error_block, panel_rows, number, targets):
        beyond = targets >= (number + 1) * block_size
        masked = jnp.where(beyond[None, None, :], panel_rows, 0.0)
        return current - jnp.einsum(
            "xrc,xcd->xrd", error_block, masked, precision=lax.Precision.HIGHEST
        )

    def record(errors, error_block, number):
        owner_rank = number // local_blocks
        offset = number % local_blocks * block_size
        previous = lax.dynamic_slice_in_dim(errors, offset, block_size, 2)
        chosen = jnp.where(owner_rank == column_rank, error_block, previous)
        return lax.dynamic_update_slice_in_dim(errors, chosen, offset, 2)

    blank = jnp.zeros(weights.shape, jnp.float32)

    def advance(number, state_pair):
        current, errors = state_pair
        error_block = block_error(own_block(current, number), number)
        errors = record(errors, error_block, number)
        current = propagate(current, error_block, panel_of(number), number, column_ids)
        return (current, errors)

    _, errors = lax.fori_loop(0, block_total, advance, (offset_weights, blank))
    row_loss = lax.psum(jnp.sum(errors * errors, axis=2), "col")
    mass = local_mass(errors[0], assign[0], code_count)[None]
    codeword_mass = lax.psum(mass, "row")
    return (errors, row_loss, codeword_mass)


def local(weights, codebook, assign, chol_upper, inv_blocks):
    count = chol_upper.shape[1] // LANES
    chips = lax.axis_size("row")
    if (
        lax.axis_size("col") == 2
        and chol_upper.shape[1] == count * LANES
        and count & (count - 1) == 0
        and chips & (chips - 1) == 0
        and chips > 1
        and chips * chol_upper.shape[1] == 2 * weights.shape[2]
    ):
        return chained(weights, codebook, assign, chol_upper, inv_blocks)
    return general(weights, codebook, assign, chol_upper, inv_blocks)


def solution(mesh):
    return jax.shard_map(
        local,
        mesh=mesh,
        in_specs=(
            P("ea", "row", "col"),
            P("ea", "col", None, None),
            P("ea", "row", "col"),
            P("ea", "row", "col"),
            P("ea", "col", None, None),
        ),
        out_specs=(P("ea", "row", "col"), P("ea", "row"), P("ea", "col", None)),
        check_vma=False,
    )
```
